256 devices in a mesh: dp: 64 (over x, z, core), tensor: 4 (over y).
Axes of the slice: x: 4, y: 4, z: 8, core: 2. Of those that a mesh axis runs over, the one named last changes fastest.
Arguments:
- grad_codes: bfloat16 [4, 64, 64, 18432], P(None, 'dp', None, 'tensor'), may hold values from -448 to 448
- exponents: int32 [4, 64, 16], P(None, 'dp'), may hold values from 7 to 10
- accumulated: bfloat16 [64, 18432], P('dp', 'tensor'), may hold values from -12 to 12
- arrival: int32 [64], replicated, may hold values from 0 to 63, each once
- bucket_of_row: int32 [64], replicated, may hold values from 0 to 15, never falling along the last dimension, each value on 1 to 8 neighbouring positions
Outputs:
- unit_codes: bfloat16 [4, 64, 18432], P(None, 'dp', 'tensor')
- bucket_peaks: float32 [4, 16], replicated
- compensated: float32 [64, 18432], P('dp', 'tensor')
The draws below stay inside these ranges and needn't reach their ends.
Inputs may be any that keep to these rules, and one draw needn't show every extreme that they name: `arrival`: each weight row appears in exactly one slot. `bucket_of_row`: bucket numbers never fall along the rows; each bucket holds 1 to 8 consecutive rows and one holds exactly 8.
All inputs are finite; a program needn't handle non-finite values.
Results may differ from the reference program's by a relative error of at most 0.001.
Values sent between devices are 32-bit elements; how exact they have to be, the bound alone decides.
No kernel may reach another device: no remote copies, remote signals or barrier semaphores. Data moves between devices by JAX's collectives and lax.ppermute only.
A program may use at most 64 MiB of HBM per device.

```python
import math
import jax
import jax.numpy as jnp
import numpy as np
from jax import lax

FF = 18432
STEPS = 4
NB = 16
ROWS = 64
REPLICAS = 64
BMOST = 8


def plant(array, rng, least, high):
    longest = array.shape.index(max(array.shape))
    spots = []
    for shift in (0, 1):
        where = [jax.random.randint(jax.random.fold_in(rng, axis), (), 0, length) for axis, length in enumerate(array.shape)]
        where[longest] = (where[longest] + shift) % array.shape[longest]
        spots.append(tuple(where))
    return array.at[spots[0]].set(least).at[spots[1]].set(high)


def raised(drawn, stream_key, source, target, blocks, factor):
    def block_of(axis_at):
        return (jnp.arange(drawn.shape[axis_at]) // (drawn.shape[axis_at] // blocks)).reshape((-1,) + (1,) * (drawn.ndim - 1 - axis_at))

    first = jax.random.permutation(stream_key, blocks)[block_of(target)]
    second = (block_of(target) + blocks // 2) % blocks
    return jnp.where((block_of(source) == first) | (block_of(source) == second), factor * drawn, drawn)


def levels(stream_key, extent, shards, low, high):
    def one(position, shards_of):
        draws = jax.random.uniform(jax.random.fold_in(jax.random.fold_in(stream_key, 6), position), (shards_of,), jnp.float32, low / len(shards), high / len(shards))
        return jnp.repeat(jnp.exp(draws), extent[position] // shards_of).reshape((-1,) + (1,) * (len(extent) - position - 1))

    factor_of = one(*shards[0])
    for cut in shards[1:]:
        factor_of = factor_of * one(*cut)
    return factor_of


def profile(amount, total, most, skew):
    loads = [(1 << 20) // math.isqrt(standing ** skew) + 1 for standing in range(2, amount + 1)]
    rest, counts = total - most - (amount - 1), [1] * (amount - 1)
    while rest > 0:
        free = [i for i in range(amount - 1) if counts[i] < most]
        whole, left = sum([loads[i] for i in free]), rest
        for i in free:
            extra = min(most - counts[i], max(1, left * loads[i] // whole), rest)
            counts[i] = counts[i] + extra
            rest = rest - extra
    return np.array([most] + counts)


def ragged(own_key, number_of, total, most, lean):
    if number_of == 2:
        one = jax.random.randint(own_key, (), max(1, total - most), min(most, total - 1) + 1)
        return jnp.stack([one, total - one])
    sizes = jnp.asarray(profile(number_of, total, most, lean), jnp.int32)
    twos = (number_of - 1) // 2
    source_of, receiver = sizes[1:1 + 2 * twos:2], sizes[2:2 + 2 * twos:2]
    room = jnp.minimum(source_of - 1, most - receiver)
    shifted = jax.random.randint(jax.random.fold_in(own_key, 1), (twos,), 0, 1 << 20) % (room + 1)
    sizes = sizes.at[1:1 + 2 * twos:2].set(source_of - shifted).at[2:2 + 2 * twos:2].set(receiver + shifted)
    return sizes[jax.random.permutation(jax.random.fold_in(own_key, 2), number_of)]


def gaussian(key, dims, deviation, most, split=(), kind=jnp.bfloat16):
    array = jax.random.normal(key, dims, jnp.float32) * deviation
    if len(split) > 0:
        array = levels(key, dims, split, -0.22, 0.18) * array
    return jnp.clip(array, min=-most, max=most).astype(kind)


def noise_with(key, extent, width, reach, pieces, heavy, held_as=jnp.bfloat16):
    drawn = width * jax.random.normal(key, extent, jnp.float32)
    if pieces:
        drawn = drawn * levels(key, extent, pieces, -0.22, 0.18)
    return jnp.clip(raised(drawn, jax.random.fold_in(key, 3), *heavy), -reach, reach).astype(held_as)


def setup_inputs(seed: int = 0) -> dict:
    key_list = jax.random.split(jax.random.key(seed), 6)
    grad_codes = noise_with(key_list[0], (STEPS, REPLICAS, ROWS, FF), 64.0, 448.0, ((1, 64), (3, 4)), (1, 2, 64, 4.0))
    exponents = plant(jax.random.randint(key_list[1], (STEPS, REPLICAS, NB), 7, 11), jax.random.fold_in(key_list[1], 1), 7, 10).astype(jnp.int32)
    accumulated = gaussian(key_list[2], (ROWS, FF), 2.0, 12.0, ((0, 64), (1, 4)))
    arrival = jax.random.permutation(key_list[3], ROWS).astype(jnp.int32)
    bucket_of_row = jnp.searchsorted(jnp.cumsum(ragged(key_list[4], NB, ROWS, BMOST, 1)), jnp.arange(ROWS), side="right").astype(jnp.int32)
    return {"grad_codes": grad_codes, "exponents": exponents, "accumulated": accumulated, "arrival": arrival, "bucket_of_row": bucket_of_row}


epsilon = 1e-6


def reference(grad_codes, exponents, accumulated, arrival, bucket_of_row):
    inverse = jnp.zeros((ROWS,), jnp.int32).at[arrival].set(jnp.arange(ROWS, dtype=jnp.int32))
    member = bucket_of_row[:, None] == jnp.arange(NB, dtype=jnp.int32)[None, :]

    def add_replica(running_sum, replica_item):
        row_block, exponent_row = replica_item
        factor = jnp.exp2(-exponent_row.astype(jnp.float32))
        factor_rows = jnp.sum(jnp.where(member, factor[None, :], jnp.float32(0.0)), axis=1)
        picked = jnp.take(row_block, inverse, axis=0).astype(jnp.float32)
        return running_sum + picked * factor_rows[:, None], None

    running = accumulated
    carried = jnp.zeros((ROWS, FF), jnp.float32)
    unit_list = []
    peak_list = []
    exact_sum = carried
    for micro_step in range(STEPS):
        reduced, _ = lax.scan(add_replica, jnp.zeros((ROWS, FF), jnp.float32),
                              (grad_codes[micro_step], exponents[micro_step]))
        adjusted = reduced - carried
        previous = running.astype(jnp.float32)
        running = lax.optimization_barrier((previous + adjusted).astype(jnp.bfloat16))
        carried = (running.astype(jnp.float32) - previous) - adjusted
        exact_sum = running.astype(jnp.float32) - carried
        row_max = jnp.max(jnp.abs(exact_sum), axis=1)
        peaks = jnp.max(jnp.where(member, row_max[:, None], jnp.float32(0.0)), axis=0)
        peak_rows = jnp.sum(jnp.where(member, peaks[None, :], jnp.float32(0.0)), axis=1)
        unit_list.append((exact_sum / (peak_rows[:, None] + epsilon)).astype(jnp.bfloat16))
        peak_list.append(peaks)
    return jnp.stack(unit_list), jnp.stack(peak_list), exact_sum
```

```python
import functools

import jax
import jax.numpy as jnp
from jax import lax
from jax.experimental import pallas as pl
from jax.experimental.pallas import tpu as pltpu
from jax.sharding import Mesh
from jax.sharding import PartitionSpec as P

NB = 16
STEPS = 4
ROWS = 64
LANES = 128
EPSILON = 1e-06

NAMES = ("a4", "b3", "a3", "b2", "a2", "b1", "a1")


def where_rows(tiles):
    half = 2 * tiles
    base, at = {}, 0
    for name in NAMES:
        base[name] = at
        at += 8 * half
    for name in ("own_a", "own_b"):
        base[name] = at
        at += 4 * half
    return base, at


def spread_kernel(tiles, place, arrival, bucket, exponents, codes, mine, send, held, sems):
    base, _ = where_rows(tiles)
    half = 2 * tiles
    x, z, c = place[0], place[1], place[2]

    def copy(rel):
        return pltpu.make_async_copy(codes.at[rel ^ (2 * (1 - c))], held.at[rel], sems.at[rel])

    for rel in range(STEPS):
        copy(rel).start()
    row = lax.broadcasted_iota(jnp.int32, (ROWS, ROWS), 0)
    lane = lax.broadcasted_iota(jnp.int32, (ROWS, ROWS), 1)
    k, g = row // 8, row % 8
    to_z = (z + k * (1 - 2 * c)) & 7
    to_x = (x + g % 4) & 3

    def row_ids(own_until):
        owner = jnp.where(k <= own_until, c, 1 - c)
        return (to_x * 8 + to_z) * 2 + (owner ^ (g // 4))

    for rel in range(STEPS):
        ids = row_ids(4 if rel < 2 else 3)
        row_bucket = jnp.sum(jnp.where(ids == lane, bucket[...], 0), axis=1, keepdims=True)
        step = rel ^ (2 * (1 - c))
        power = exponents[pl.ds(step, 1), :]
        mask = row_bucket == lax.broadcasted_iota(jnp.int32, (ROWS, NB), 1)
        power = jnp.sum(jnp.where(mask, power, 0), axis=1, keepdims=True)
        factor = jnp.ones((ROWS, 1), jnp.float32)
        for bit in range(6):
            factor = factor * jnp.where((power >> bit) & 1 == 1, 2.0 ** -(2**bit), 1.0)
        pick = jnp.where(ids == arrival[...], factor, 0.0).astype(jnp.bfloat16)
        copy(rel).wait()
        h = rel % 2
        mine_half, send_half = ("a", "b") if rel < 2 else ("b", "a")
        width = 2 * LANES
        for block in range(tiles * LANES // width):
            part = jnp.dot(
                pick,
                held[rel, :, block * width : (block + 1) * width],
                preferred_element_type=jnp.float32,
            )
            for sub in range(2):
                at = h * tiles + 2 * block + sub
                for group in range(8):
                    piece = part[group * 8 : group * 8 + 8, sub * LANES : (sub + 1) * LANES]
                    if group == 0:
                        mine[pl.ds(base["own_" + mine_half] + at, 4, half), :] = piece[0:4]
                        send[pl.ds(base["own_" + send_half] + at, 4, half), :] = piece[4:8]
                    elif group < 4 or (group == 4 and rel < 2):
                        mine[pl.ds(base[mine_half + str(group)] + at, 8, half), :] = piece
                    else:
                        send[pl.ds(base[send_half + str(8 - group)] + at, 8, half), :] = piece


def spread(place, arrival, bucket, exponents, codes):
    steps, rows, columns = codes.shape
    tiles = columns // LANES
    _, total = where_rows(tiles)
    shape = jax.ShapeDtypeStruct((total, LANES), jnp.float32)
    vmem = pl.BlockSpec(memory_space=pltpu.VMEM)
    return pl.pallas_call(
        functools.partial(spread_kernel, tiles),
        out_shape=(shape, shape),
        in_specs=[
            pl.BlockSpec(memory_space=pltpu.SMEM),
            vmem,
            vmem,
            vmem,
            pl.BlockSpec(memory_space=pl.ANY),
        ],
        out_specs=(vmem, vmem),
        scratch_shapes=[
            pltpu.VMEM((steps, rows, columns), codes.dtype),
            pltpu.SemaphoreType.DMA((steps,)),
        ],
        name="spread",
    )(place, arrival, bucket, exponents, codes)


def join_kernel(half, own_m, own_r, ra, rb, back, *outs):
    both = 4 * half
    for k in range(4):
        rows = slice(k * half, (k + 1) * half)
        other = slice(both + k * half, both + (k + 1) * half)
        outs[k][0:half] = own_m[rows] + own_r[rows] + ra[rows] + back[other]
        outs[k][half : 2 * half] = own_m[other] + own_r[other] + rb[rows] + back[rows]


def chain_kernel(tiles, place, bucket, t0, t1, t2, t3, start, exact, compensated, peaks):
    c = place[2]
    mine = bucket[(place[0] * 8 + place[1]) * 2 + c]
    total = t0[...] + t1[...] + t2[...] + t3[...]
    running = start[...].astype(jnp.float32)
    carried = jnp.zeros_like(running)
    lane = lax.broadcasted_iota(jnp.int32, (1, LANES), 1)
    table = jnp.zeros((1, LANES), jnp.float32)
    for step in range(STEPS):
        first, second = (step ^ 2) * tiles, step * tiles
        reduced = jnp.where(c == 0, total[first : first + tiles], total[second : second + tiles])
        adjusted = reduced - carried
        new = (running + adjusted).astype(jnp.bfloat16).astype(jnp.float32)
        carried = (new - running) - adjusted
        running = new
        value = running - carried
        peak = jnp.max(jnp.max(jnp.abs(value), axis=0, keepdims=True), axis=1, keepdims=True)
        table = jnp.where(lane == step * NB + mine, peak, table)
        for t in range(tiles):
            exact[step : step + 1, t * LANES : (t + 1) * LANES] = value[t : t + 1]
            if step == STEPS - 1:
                compensated[:, t * LANES : (t + 1) * LANES] = value[t : t + 1]
    peaks[...] = table


def scale_kernel(place, bucket, exact, tables, units, peaks):
    mine = bucket[(place[0] * 8 + place[1]) * 2 + place[2]]
    table = jnp.max(tables[...], axis=0, keepdims=True)
    lane = lax.broadcasted_iota(jnp.int32, (STEPS, LANES), 1)
    step = lax.broadcasted_iota(jnp.int32, (STEPS, LANES), 0)
    spot = lane == step * NB + mine
    peak = jnp.max(jnp.where(spot, jnp.broadcast_to(table, spot.shape), 0.0), axis=1, keepdims=True)
    units[...] = (exact[...] / (peak + EPSILON)).astype(units.dtype)
    for s in range(STEPS):
        peaks[s : s + 1, :] = table[:, s * NB : (s + 1) * NB]


def on_device(grad_codes, exponents, accumulated, arrival, bucket_of_row):
    columns = accumulated.shape[1]
    tiles = columns // LANES
    half = 2 * tiles
    base, _ = where_rows(tiles)
    place = jnp.stack([lax.axis_index("x"), lax.axis_index("z"), lax.axis_index("c")])
    nz = lax.axis_size("z")
    vmem = pl.BlockSpec(memory_space=pltpu.VMEM)
    smem = pl.BlockSpec(memory_space=pltpu.SMEM)

    mine, send = spread(
        place, arrival[None, :], bucket_of_row[None, :], exponents[:, 0, :], grad_codes[:, 0]
    )
    swap = [(0, 1), (1, 0)]
    got = lax.ppermute(send, "c", swap)

    def part(name):
        rows = slice(base[name], base[name] + 8 * half)
        return mine[rows] + got[rows]

    turn = []
    for z in range(nz):
        turn.append((2 * z, 2 * ((z + 1) % nz)))
        turn.append((2 * z + 1, 2 * ((z - 1) % nz) + 1))
    ring = functools.partial(lax.ppermute, axis_name=("z", "c"), perm=turn)
    ra = ring(part("a4"))
    rb = ring(part("b3"))
    ra = ring(part("a3") + ra)
    rb = ring(part("b2") + rb)
    ra = ring(part("a2") + ra)
    rb = ring(part("b1") + rb)
    ra = ring(part("a1") + ra)
    cut = 4 * half
    back = lax.ppermute(jnp.concatenate([ra[cut:], rb[cut:]]), "c", swap)
    own = base["own_a"]
    piece = jax.ShapeDtypeStruct((2 * half, LANES), jnp.float32)
    pieces = pl.pallas_call(
        functools.partial(join_kernel, half),
        out_shape=(piece,) * 4,
        in_specs=[vmem] * 5,
        out_specs=(vmem,) * 4,
        name="join",
    )(mine[own:], got[own:], ra[:cut], rb[:cut], back)
    totals = [pieces[0]]
    for k in range(1, 4):
        totals.append(lax.ppermute(pieces[k], "x", [(i, (i + k) % 4) for i in range(4)]))
    exact, compensated, table = pl.pallas_call(
        functools.partial(chain_kernel, tiles),
        out_shape=(
            jax.ShapeDtypeStruct((STEPS, columns), jnp.float32),
            jax.ShapeDtypeStruct((1, columns), jnp.float32),
            jax.ShapeDtypeStruct((1, LANES), jnp.float32),
        ),
        in_specs=[smem, smem] + [vmem] * 5,
        out_specs=(vmem,) * 3,
        name="chain",
    )(place, bucket_of_row, *totals, accumulated.reshape(tiles, LANES))
    table = jnp.maximum(table, lax.ppermute(table, "c", swap))
    count = lax.axis_size(("x", "z", "y"))
    copies = jnp.broadcast_to(table[None], (count, 1, LANES))
    tables = lax.all_to_all(copies, ("x", "z", "y"), 0, 0, tiled=True)
    units, peaks = pl.pallas_call(
        scale_kernel,
        out_shape=(
            jax.ShapeDtypeStruct((STEPS, columns), jnp.bfloat16),
            jax.ShapeDtypeStruct((STEPS, NB), jnp.float32),
        ),
        in_specs=[smem, smem] + [vmem] * 2,
        out_specs=(vmem,) * 2,
        name="scale",
    )(place, bucket_of_row, exact, tables.reshape(count, LANES))
    return units[:, None, :], peaks, compensated


def solution(mesh):
    finer = Mesh(mesh.devices.reshape(4, 8, 2, mesh.shape["tensor"]), ("x", "z", "c", "y"))
    dp = ("x", "z", "c")
    in_specs = (P(None, dp, None, "y"), P(None, dp, None), P(dp, "y"), P(), P())
    out_specs = (P(None, dp, "y"), P(), P(dp, "y"))
    return jax.shard_map(
        on_device, mesh=finer, in_specs=in_specs, out_specs=out_specs, check_vma=False
    )
```

```python
import functools

import jax
import jax.numpy as jnp
from jax import lax
from jax.experimental import pallas as pl
from jax.experimental.pallas import tpu as pltpu
from jax.sharding import Mesh
from jax.sharding import PartitionSpec as P


NB = 16
STEPS = 4
ROWS = 64
LANES = 128
EPSILON = 1e-06

NAMES = ("a4", "b3", "a3", "b2", "a2", "b1", "a1")
EARLY = ("a4", "b3")


def room(mib):
    return pltpu.CompilerParams(vmem_limit_bytes=mib * 2**20)


def where_rows(tiles):
    half = 2 * tiles
    base, sizes = {}, [0, 0]
    for name in NAMES + ("own_a", "own_b"):
        late = int(name not in EARLY)
        base[name] = (late, sizes[late])
        sizes[late] += (4 if name.startswith("own") else 8) * half
    return base, sizes


def spread_kernel(tiles, place, arrival, bucket, exponents, codes, mine0, mine1, send0, send1, held, sems):
    base, _ = where_rows(tiles)
    half = 2 * tiles
    x, z, c = place[0], place[1], place[2]

    def put(outs, name, at, count, value):
        late, first = base[name]
        outs[late][pl.ds(first + at, count, half), :] = value

    mine, send = (mine0, mine1), (send0, send1)

    def copy(rel):
        return pltpu.make_async_copy(codes.at[rel ^ (2 * (1 - c))], held.at[rel], sems.at[rel])

    for rel in range(STEPS):
        copy(rel).start()
    row = lax.broadcasted_iota(jnp.int32, (ROWS, ROWS), 0)
    lane = lax.broadcasted_iota(jnp.int32, (ROWS, ROWS), 1)
    k, g = row // 8, row % 8
    to_z = (z + k * (1 - 2 * c)) & 7
    to_x = (x + g % 4) & 3

    def row_ids(own_until):
        owner = jnp.where(k <= own_until, c, 1 - c)
        return (to_x * 8 + to_z) * 2 + (owner ^ (g // 4))

    for rel in range(STEPS):
        ids = row_ids(4 if rel < 2 else 3)
        row_bucket = jnp.sum(jnp.where(ids == lane, bucket[...], 0), axis=1, keepdims=True)
        step = rel ^ (2 * (1 - c))
        power = exponents[pl.ds(step, 1), :]
        mask = row_bucket == lax.broadcasted_iota(jnp.int32, (ROWS, NB), 1)
        power = jnp.sum(jnp.where(mask, power, 0), axis=1, keepdims=True)
        factor = jnp.ones((ROWS, 1), jnp.float32)
        for bit in range(6):
            factor = factor * jnp.where((power >> bit) & 1 == 1, 2.0 ** -(2**bit), 1.0)
        pick = jnp.where(ids == arrival[...], factor, 0.0).astype(jnp.bfloat16)
        copy(rel).wait()
        h = rel % 2
        mine_half, send_half = ("a", "b") if rel < 2 else ("b", "a")
        width = 2 * LANES
        for block in range(tiles * LANES // width):
            part = jnp.dot(
                pick,
                held[rel, :, block * width : (block + 1) * width],
                preferred_element_type=jnp.float32,
            )
            for sub in range(2):
                at = h * tiles + 2 * block + sub
                for group in range(8):
                    piece = part[group * 8 : group * 8 + 8, sub * LANES : (sub + 1) * LANES]
                    if group == 0:
                        put(mine, "own_" + mine_half, at, 4, piece[0:4])
                        put(send, "own_" + send_half, at, 4, piece[4:8])
                    elif group < 4 or (group == 4 and rel < 2):
                        put(mine, mine_half + str(group), at, 8, piece)
                    else:
                        put(send, send_half + str(8 - group), at, 8, piece)


def spread(place, arrival, bucket, exponents, codes):
    steps, rows, columns = codes.shape
    tiles = columns // LANES
    shapes = tuple(
        jax.ShapeDtypeStruct((size, LANES), jnp.float32) for size in where_rows(tiles)[1]
    )
    vmem = pl.BlockSpec(memory_space=pltpu.VMEM)
    return pl.pallas_call(
        functools.partial(spread_kernel, tiles),
        out_shape=shapes + shapes,
        in_specs=[
            pl.BlockSpec(memory_space=pltpu.SMEM),
            vmem,
            vmem,
            vmem,
            pl.BlockSpec(memory_space=pltpu.HBM),
        ],
        out_specs=(vmem,) * 4,
        scratch_shapes=[
            pltpu.VMEM((steps, rows, columns), codes.dtype),
            pltpu.SemaphoreType.DMA((steps,)),
        ],
        compiler_params=room(16),
        name="spread",
    )(place, arrival, bucket, exponents, codes)


def add_kernel(first, *refs):
    *ins, out = refs
    rows = slice(first, first + out.shape[0])
    total = ins[0][rows] + ins[1][rows]
    if len(ins) == 3:
        total = total + ins[2][...]
    out[...] = total


def join_kernel(half, own_a, own_b, mine, got, ra, rb, back_a, back_b, *outs):
    for k in range(4):
        rows = slice(k * half, (k + 1) * half)
        other = slice((k + 4) * half, (k + 5) * half)
        at = slice(own_a + k * half, own_a + (k + 1) * half)
        outs[k][0:half] = mine[at] + got[at] + ra[rows] + back_b[other]
        at = slice(own_b + k * half, own_b + (k + 1) * half)
        outs[k][half : 2 * half] = mine[at] + got[at] + rb[rows] + back_a[other]


def chain_kernel(tiles, place, bucket, t0, t1, t2, t3, start, exact, compensated, peaks):
    c = place[2]
    mine = bucket[(place[0] * 8 + place[1]) * 2 + c]
    total = t0[...] + t1[...] + t2[...] + t3[...]
    running = start[...].astype(jnp.float32)
    carried = jnp.zeros_like(running)
    lane = lax.broadcasted_iota(jnp.int32, (1, LANES), 1)
    table = jnp.zeros((1, LANES), jnp.float32)
    for step in range(STEPS):
        first, second = (step ^ 2) * tiles, step * tiles
        reduced = jnp.where(c == 0, total[first : first + tiles], total[second : second + tiles])
        adjusted = reduced - carried
        new = (running + adjusted).astype(jnp.bfloat16).astype(jnp.float32)
        carried = (new - running) - adjusted
        running = new
        value = running - carried
        peak = jnp.max(jnp.max(jnp.abs(value), axis=0, keepdims=True), axis=1, keepdims=True)
        table = jnp.where(lane == step * NB + mine, peak, table)
        for t in range(tiles):
            exact[step : step + 1, t * LANES : (t + 1) * LANES] = value[t : t + 1]
            if step == STEPS - 1:
                compensated[:, t * LANES : (t + 1) * LANES] = value[t : t + 1]
    peaks[...] = table


def scale_kernel(place, bucket, exact, tables, units, peaks):
    mine = bucket[(place[0] * 8 + place[1]) * 2 + place[2]]
    table = jnp.max(tables[...], axis=0, keepdims=True)
    lane = lax.broadcasted_iota(jnp.int32, (STEPS, LANES), 1)
    step = lax.broadcasted_iota(jnp.int32, (STEPS, LANES), 0)
    spot = lane == step * NB + mine
    peak = jnp.max(jnp.where(spot, jnp.broadcast_to(table, spot.shape), 0.0), axis=1, keepdims=True)
    units[...] = (exact[...] / (peak + EPSILON)).astype(units.dtype)
    for s in range(STEPS):
        peaks[s : s + 1, :] = table[:, s * NB : (s + 1) * NB]


def on_device(grad_codes, exponents, accumulated, arrival, bucket_of_row):
    columns = accumulated.shape[1]
    tiles = columns // LANES
    half = 2 * tiles
    base, _ = where_rows(tiles)
    place = jnp.stack([lax.axis_index("x"), lax.axis_index("z"), lax.axis_index("c")])
    nz = lax.axis_size("z")
    vmem = pl.BlockSpec(memory_space=pltpu.VMEM)
    smem = pl.BlockSpec(memory_space=pltpu.SMEM)

    *mine, send0, send1 = spread(
        place, arrival[None, :], bucket_of_row[None, :], exponents[:, 0, :], grad_codes[:, 0]
    )
    swap = [(0, 1), (1, 0)]
    got = [lax.ppermute(send0, "c", swap), lax.ppermute(send1, "c", swap)]
    turn = []
    for z in range(nz):
        turn.append((2 * z, 2 * ((z + 1) % nz)))
        turn.append((2 * z + 1, 2 * ((z - 1) % nz) + 1))

    arrived = {"a": (), "b": ()}
    for name in NAMES:
        late, first = base[name]
        ins = (mine[late], got[late]) + arrived[name[0]]
        held = pl.pallas_call(
            functools.partial(add_kernel, first),
            out_shape=jax.ShapeDtypeStruct((8 * half, LANES), jnp.float32),
            in_specs=[vmem] * len(ins),
            out_specs=vmem,
            compiler_params=room(4),
            name="add",
        )(*ins)
        arrived[name[0]] = (lax.ppermute(held, ("z", "c"), turn),)
    (ra,), (rb,) = arrived["a"], arrived["b"]
    back_b = lax.ppermute(rb, "c", swap)
    back_a = lax.ppermute(ra, "c", swap)
    piece = jax.ShapeDtypeStruct((2 * half, LANES), jnp.float32)
    pieces = pl.pallas_call(
        functools.partial(join_kernel, half, base["own_a"][1], base["own_b"][1]),
        out_shape=(piece,) * 4,
        in_specs=[vmem] * 6,
        out_specs=(vmem,) * 4,
        compiler_params=room(4),
        name="join",
    )(mine[1], got[1], ra, rb, back_a, back_b)
    totals = [pieces[0]]
    for k in range(1, 4):
        totals.append(lax.ppermute(pieces[k], "x", [(i, (i + k) % 4) for i in range(4)]))
    exact, compensated, table = pl.pallas_call(
        functools.partial(chain_kernel, tiles),
        out_shape=(
            jax.ShapeDtypeStruct((STEPS, columns), jnp.float32),
            jax.ShapeDtypeStruct((1, columns), jnp.float32),
            jax.ShapeDtypeStruct((1, LANES), jnp.float32),
        ),
        in_specs=[smem, smem] + [vmem] * 5,
        out_specs=(vmem,) * 3,
        compiler_params=room(4),
        name="chain",
    )(place, bucket_of_row, *totals, accumulated.reshape(tiles, LANES))
    table = jnp.maximum(table, lax.ppermute(table, "c", swap))
    count = lax.axis_size(("x", "z", "y"))
    copies = jnp.broadcast_to(table[None], (count, 1, LANES))
    tables = lax.all_to_all(copies, ("x", "z", "y"), 0, 0, tiled=True)
    units, peaks = pl.pallas_call(
        scale_kernel,
        out_shape=(
            jax.ShapeDtypeStruct((STEPS, columns), jnp.bfloat16),
            jax.ShapeDtypeStruct((STEPS, NB), jnp.float32),
        ),
        in_specs=[smem, smem] + [vmem] * 2,
        out_specs=(vmem,) * 2,
        compiler_params=room(4),
        name="scale",
    )(place, bucket_of_row, exact, tables.reshape(count, LANES))
    return units[:, None, :], peaks, compensated


def solution(mesh):
    finer = Mesh(mesh.devices.reshape(4, 8, 2, mesh.shape["tensor"]), ("x", "z", "c", "y"))
    dp = ("x", "z", "c")
    in_specs = (P(None, dp, None, "y"), P(None, dp, None), P(dp, "y"), P(), P())
    out_specs = (P(None, dp, "y"), P(), P(dp, "y"))

    return jax.shard_map(
        on_device, mesh=finer, in_specs=in_specs, out_specs=out_specs, check_vma=False
    )
```

```python
import functools

import jax
import jax.numpy as jnp
from jax import lax
from jax.experimental import pallas as pl
from jax.experimental.pallas import tpu as pltpu
from jax.sharding import Mesh
from jax.sharding import PartitionSpec as P


NB = 16
STEPS = 4
ROWS = 64
LANES = 128
EPSILON = 1e-06

PIECES = tuple(
    (hops - (rel >= 2), rel) for hops in (4, 3, 2, 1) for rel in range(STEPS) if hops - (rel >= 2) > 0
)
EARLY = PIECES[:STEPS]


def room(mib):
    return pltpu.CompilerParams(vmem_limit_bytes=mib * 2**20)


def where_rows(tiles):
    base, sizes = {}, [0, 0]
    for piece in PIECES + tuple((0, rel) for rel in range(STEPS)):
        late = int(piece not in EARLY)
        base[piece] = (late, sizes[late])
        sizes[late] += (8 if piece[0] else 4) * tiles
    return base, sizes


def group_order(rel):
    first = [4, 5] if rel < 2 else [3, 4]
    return first + [k for k in range(8) if k not in first]


def picks_kernel(place, table, picks):
    x, z, c = place[0], place[1], place[2]
    shape = (ROWS, ROWS)
    group = lax.broadcasted_iota(jnp.int32, shape, 0) // 8
    g = lax.broadcasted_iota(jnp.int32, shape, 0) % 8
    lane = lax.broadcasted_iota(jnp.int32, shape, 1)
    arrival, bucket = table[0:1, 0:ROWS], table[0:1, ROWS : 2 * ROWS]
    exponents = table[1:2, 0:ROWS]
    to_x = x ^ (g % 4)
    for rel in range(STEPS):
        k = jnp.zeros(shape, jnp.int32)
        for index, value in enumerate(group_order(rel)):
            k = jnp.where(group == index, value, k)
        to_z = (z + k * (1 - 2 * c)) & 7
        owner = jnp.where(k <= (4 if rel < 2 else 3), c, 1 - c)
        ids = (to_x * 8 + to_z) * 2 + (owner ^ (g // 4))
        row_bucket = jnp.sum(jnp.where(ids == lane, bucket, 0), axis=1, keepdims=True)
        step = rel ^ (2 * (1 - c))
        power = jnp.sum(
            jnp.where(row_bucket + step * NB == lane, exponents, 0), axis=1, keepdims=True
        )
        factor = jnp.ones((ROWS, 1), jnp.float32)
        for bit in range(6):
            factor = factor * jnp.where((power >> bit) & 1 == 1, 2.0 ** -(2**bit), 1.0)
        picks[rel] = jnp.where(ids == arrival, factor, 0.0).astype(jnp.bfloat16)


def spread_kernel(tiles, late, place, picks, codes, mine, send):
    base, _ = where_rows(tiles)
    c = place[2]
    width = 2 * LANES
    rows = slice(16, ROWS) if late else slice(0, 16)

    def put(out, piece, at, value):
        assert base[piece][0] == late
        out[pl.ds(base[piece][1] + at, value.shape[0], tiles), :] = value

    for rel in range(STEPS):
        order = group_order(rel)[2:] if late else group_order(rel)[:2]
        pick = picks[rel, rows, :]
        step = rel ^ (2 * (1 - c))
        for block in range(tiles * LANES // width):
            part = jnp.dot(
                pick,
                codes[step, :, block * width : (block + 1) * width],
                preferred_element_type=jnp.float32,
            )
            for sub in range(2):
                at = 2 * block + sub
                for index, k in enumerate(order):
                    piece = part[index * 8 : index * 8 + 8, sub * LANES : (sub + 1) * LANES]
                    if k == 0:
                        put(mine, (0, rel), at, piece[0:4])
                        put(send, (0, rel ^ 2), at, piece[4:8])
                    elif (k, rel) in base:
                        put(mine, (k, rel), at, piece)
                    else:
                        put(send, (8 - k, rel ^ 2), at, piece)


def spread(late, place, picks, codes):
    tiles = codes.shape[2] // LANES
    shape = jax.ShapeDtypeStruct((where_rows(tiles)[1][late], LANES), jnp.float32)
    vmem = pl.BlockSpec(memory_space=pltpu.VMEM)
    return pl.pallas_call(
        functools.partial(spread_kernel, tiles, late),
        out_shape=(shape, shape),
        in_specs=[pl.BlockSpec(memory_space=pltpu.SMEM), vmem, vmem],
        out_specs=(vmem, vmem),
        compiler_params=room(8),
        name="spread",
    )(place, picks, codes)


def add_kernel(first, *refs):
    *ins, out = refs
    rows = slice(first, first + out.shape[0])
    total = ins[0][rows] + ins[1][rows]
    if len(ins) == 3:
        total = total + ins[2][...]
    out[...] = total


def join_kernel(tiles, own, mine, got, r0, r1, r2, r3, b0, b1, b2, b3, *outs):
    ring, back = (r0, r1, r2, r3), (b0, b1, b2, b3)
    for k in range(4):
        rows = slice(k * tiles, (k + 1) * tiles)
        other = slice((k + 4) * tiles, (k + 5) * tiles)
        for rel in range(STEPS):
            at = slice(own[rel] + k * tiles, own[rel] + (k + 1) * tiles)
            outs[k][rel * tiles : (rel + 1) * tiles] = (
                mine[at] + got[at] + ring[rel][rows] + back[rel ^ 2][other]
            )


def chain_kernel(tiles, place, bucket, t0, t1, t2, t3, start, exact, peaks):
    c = place[2]
    mine = bucket[(place[0] * 8 + place[1]) * 2 + c]
    total = t0[...] + t1[...] + t2[...] + t3[...]
    running = start[...].astype(jnp.float32)
    carried = jnp.zeros_like(running)
    lane = lax.broadcasted_iota(jnp.int32, (1, LANES), 1)
    table = jnp.zeros((1, LANES), jnp.float32)
    for step in range(STEPS):
        first, second = (step ^ 2) * tiles, step * tiles
        reduced = jnp.where(c == 0, total[first : first + tiles], total[second : second + tiles])
        adjusted = reduced - carried
        new = (running + adjusted).astype(jnp.bfloat16).astype(jnp.float32)
        carried = (new - running) - adjusted
        running = new
        value = running - carried
        peak = jnp.max(jnp.max(jnp.abs(value), axis=0, keepdims=True), axis=1, keepdims=True)
        table = jnp.where(lane == step * NB + mine, peak, table)
        for t in range(tiles):
            exact[step : step + 1, t * LANES : (t + 1) * LANES] = value[t : t + 1]
    peaks[...] = table


def scale_kernel(place, bucket, exact, tables, units, peaks, compensated):
    mine = bucket[(place[0] * 8 + place[1]) * 2 + place[2]]
    table = jnp.max(tables[...], axis=0, keepdims=True)
    lane = lax.broadcasted_iota(jnp.int32, (STEPS, LANES), 1)
    step = lax.broadcasted_iota(jnp.int32, (STEPS, LANES), 0)
    spot = lane == step * NB + mine
    peak = jnp.max(jnp.where(spot, jnp.broadcast_to(table, spot.shape), 0.0), axis=1, keepdims=True)
    compensated[...] = exact[STEPS - 1 : STEPS, :]
    units[...] = (exact[...] / (peak + EPSILON)).astype(units.dtype)
    for s in range(STEPS):
        peaks[s : s + 1, :] = table[:, s * NB : (s + 1) * NB]


def on_device(grad_codes, exponents, accumulated, arrival, bucket_of_row):
    columns = accumulated.shape[1]
    tiles = columns // LANES
    base, _ = where_rows(tiles)
    place = jnp.stack([lax.axis_index("x"), lax.axis_index("z"), lax.axis_index("c")])
    nz = lax.axis_size("z")
    vmem = pl.BlockSpec(memory_space=pltpu.VMEM)
    smem = pl.BlockSpec(memory_space=pltpu.SMEM)
    codes = grad_codes[:, 0]

    words = jnp.concatenate([arrival, bucket_of_row, exponents.reshape(-1), jnp.zeros_like(arrival)])
    picks = pl.pallas_call(
        picks_kernel,
        out_shape=jax.ShapeDtypeStruct((STEPS, ROWS, ROWS), jnp.bfloat16),
        in_specs=[smem, vmem],
        out_specs=vmem,
        compiler_params=room(4),
        name="picks",
    )(place, words.reshape(2, LANES))

    swap = [(0, 1), (1, 0)]
    mine0, send0 = spread(0, place, picks, codes)
    got0 = lax.ppermute(send0, "c", swap)
    mine1, send1 = spread(1, place, picks, codes)
    got1 = lax.ppermute(send1, "c", swap)
    mine, got = (mine0, mine1), (got0, got1)
    turn = []
    for z in range(nz):
        turn.append((2 * z, 2 * ((z + 1) % nz)))
        turn.append((2 * z + 1, 2 * ((z - 1) % nz) + 1))

    ring = [()] * STEPS
    for hops, rel in PIECES:
        late, first = base[hops, rel]
        ins = (mine[late], got[late]) + ring[rel]
        held = pl.pallas_call(
            functools.partial(add_kernel, first),
            out_shape=jax.ShapeDtypeStruct((8 * tiles, LANES), jnp.float32),
            in_specs=[vmem] * len(ins),
            out_specs=vmem,
            compiler_params=room(4),
            name="add",
        )(*ins)
        ring[rel] = (lax.ppermute(held, ("z", "c"), turn),)
    ring = [arrived for (arrived,) in ring]
    back = [lax.ppermute(arrived, "c", swap) for arrived in ring]
    piece = jax.ShapeDtypeStruct((STEPS * tiles, LANES), jnp.float32)
    own = tuple(base[0, rel][1] for rel in range(STEPS))
    pieces = pl.pallas_call(
        functools.partial(join_kernel, tiles, own),
        out_shape=(piece,) * 4,
        in_specs=[vmem] * 10,
        out_specs=(vmem,) * 4,
        compiler_params=room(4),
        name="join",
    )(mine1, got1, *ring, *back)
    totals = [pieces[0]]
    for k in range(1, 4):
        totals.append(lax.ppermute(pieces[k], "x", [(i, i ^ k) for i in range(4)]))
    exact, table = pl.pallas_call(
        functools.partial(chain_kernel, tiles),
        out_shape=(
            jax.ShapeDtypeStruct((STEPS, columns), jnp.float32),
            jax.ShapeDtypeStruct((1, LANES), jnp.float32),
        ),
        in_specs=[smem, smem] + [vmem] * 5,
        out_specs=(vmem,) * 2,
        compiler_params=room(4),
        name="chain",
    )(place, bucket_of_row, *totals, accumulated.reshape(tiles, LANES))
    table = jnp.maximum(table, lax.ppermute(table, "c", swap))
    count = lax.axis_size(("x", "z", "y"))
    copies = jnp.broadcast_to(table[None], (count, 1, LANES))
    tables = lax.all_to_all(copies, ("x", "z", "y"), 0, 0, tiled=True)
    units, peaks, compensated = pl.pallas_call(
        scale_kernel,
        out_shape=(
            jax.ShapeDtypeStruct((STEPS, columns), jnp.bfloat16),
            jax.ShapeDtypeStruct((STEPS, NB), jnp.float32),
            jax.ShapeDtypeStruct((1, columns), jnp.float32),
        ),
        in_specs=[smem, smem] + [vmem] * 2,
        out_specs=(vmem,) * 3,
        compiler_params=room(4),
        name="scale",
    )(place, bucket_of_row, exact, tables.reshape(count, LANES))
    return units[:, None, :], peaks, compensated


def solution(mesh):
    finer = Mesh(mesh.devices.reshape(4, 8, 2, mesh.shape["tensor"]), ("x", "z", "c", "y"))
    dp = ("x", "z", "c")
    in_specs = (P(None, dp, None, "y"), P(None, dp, None), P(dp, "y"), P(), P())
    out_specs = (P(None, dp, "y"), P(), P(dp, "y"))

    return jax.shard_map(
        on_device, mesh=finer, in_specs=in_specs, out_specs=out_specs, check_vma=False
    )
```

```python
import functools

import jax
import jax.numpy as jnp
from jax import lax
from jax.experimental import pallas as pl
from jax.experimental.pallas import tpu as pltpu
from jax.sharding import Mesh
from jax.sharding import PartitionSpec as P


NB = 16
STEPS = 4
ROWS = 64
LANES = 128
EPSILON = 1e-06

PIECES = tuple(
    (hops - (rel >= 2), rel) for hops in (4, 3, 2, 1) for rel in range(STEPS) if hops - (rel >= 2) > 0
)
EARLY = PIECES[:STEPS]


def room(mib):
    return pltpu.CompilerParams(vmem_limit_bytes=mib * 2**20)


def where_rows(tiles):
    base, sizes = {}, [0, 0]
    for piece in PIECES + tuple((0, rel) for rel in range(STEPS)):
        late = int(piece not in EARLY)
        base[piece] = (late, sizes[late])
        sizes[late] += (8 if piece[0] else 4) * tiles
    return base, sizes


def group_order(rel):
    first = [4, 5] if rel < 2 else [3, 4]
    return first + [k for k in range(8) if k not in first]


def picks_kernel(place, table, picks):
    x, z, c = place[0], place[1], place[2]
    shape = (ROWS, ROWS)
    group = lax.broadcasted_iota(jnp.int32, shape, 0) // 8
    g = lax.broadcasted_iota(jnp.int32, shape, 0) % 8
    lane = lax.broadcasted_iota(jnp.int32, shape, 1)
    arrival, bucket = table[STEPS : STEPS + 1, 0:ROWS], table[STEPS + 1 : STEPS + 2, 0:ROWS]
    to_x = x ^ (g % 4)
    for rel in range(STEPS):
        k = jnp.zeros(shape, jnp.int32)
        for index, value in enumerate(group_order(rel)):
            k = jnp.where(group == index, value, k)
        to_z = (z + k * (1 - 2 * c)) & 7
        owner = jnp.where(k <= (4 if rel < 2 else 3), c, 1 - c)
        ids = (to_x * 8 + to_z) * 2 + (owner ^ (g // 4))
        row_bucket = jnp.sum(jnp.where(ids == lane, bucket, 0), axis=1, keepdims=True)
        exponents = jnp.where(c == 0, table[rel ^ 2, 0:ROWS][None], table[rel, 0:ROWS][None])
        power = jnp.sum(jnp.where(row_bucket == lane, exponents, 0), axis=1, keepdims=True)
        factor = jnp.ones((ROWS, 1), jnp.float32)
        for bit in range(6):
            factor = factor * jnp.where((power >> bit) & 1 == 1, 2.0 ** -(2**bit), 1.0)
        picks[rel] = jnp.where(ids == arrival, factor, 0.0).astype(jnp.bfloat16)


def spread_kernel(tiles, late, place, picks, codes, mine, send):
    base, _ = where_rows(tiles)
    c = place[2]
    width = 2 * LANES
    rows = slice(16, ROWS) if late else slice(0, 16)

    def put(out, piece, at, value):
        assert base[piece][0] == late
        out[pl.ds(base[piece][1] + at, value.shape[0], tiles), :] = value

    for rel in range(STEPS):
        order = group_order(rel)[2:] if late else group_order(rel)[:2]
        pick = picks[rel, rows, :]
        step = rel ^ (2 * (1 - c))
        for block in range(tiles * LANES // width):
            part = jnp.dot(
                pick,
                codes[step, :, block * width : (block + 1) * width],
                preferred_element_type=jnp.float32,
            )
            for sub in range(2):
                at = 2 * block + sub
                for index, k in enumerate(order):
                    piece = part[index * 8 : index * 8 + 8, sub * LANES : (sub + 1) * LANES]
                    if k == 0:
                        put(mine, (0, rel), at, piece[0:4])
                        put(send, (0, rel ^ 2), at, piece[4:8])
                    elif (k, rel) in base:
                        put(mine, (k, rel), at, piece)
                    else:
                        put(send, (8 - k, rel ^ 2), at, piece)


def spread(late, place, picks, codes):
    tiles = codes.shape[2] // LANES
    shape = jax.ShapeDtypeStruct((where_rows(tiles)[1][late], LANES), jnp.float32)
    vmem = pl.BlockSpec(memory_space=pltpu.VMEM)
    return pl.pallas_call(
        functools.partial(spread_kernel, tiles, late),
        out_shape=(shape, shape),
        in_specs=[pl.BlockSpec(memory_space=pltpu.SMEM), vmem, vmem],
        out_specs=(vmem, vmem),
        compiler_params=room(8),
        name="spread",
    )(place, picks, codes)


def add_kernel(first, *refs):
    *ins, out = refs
    rows = slice(first, first + out.shape[0])
    total = ins[0][rows] + ins[1][rows]
    if len(ins) == 3:
        total = total + ins[2][...]
    out[...] = total


def join_kernel(tiles, own, mine, got, r0, r1, r2, r3, b0, b1, b2, b3, *outs):
    ring, back = (r0, r1, r2, r3), (b0, b1, b2, b3)
    for k in range(4):
        rows = slice(k * tiles, (k + 1) * tiles)
        other = slice((k + 4) * tiles, (k + 5) * tiles)
        for rel in range(STEPS):
            at = slice(own[rel] + k * tiles, own[rel] + (k + 1) * tiles)
            outs[k][rel * tiles : (rel + 1) * tiles] = (
                mine[at] + got[at] + ring[rel][rows] + back[rel ^ 2][other]
            )


def chain_kernel(tiles, place, bucket, t0, t1, t2, t3, start, exact, peaks):
    c = place[2]
    mine = bucket[(place[0] * 8 + place[1]) * 2 + c]
    total = t0[...] + t1[...] + t2[...] + t3[...]
    running = start[...].astype(jnp.float32)
    carried = jnp.zeros_like(running)
    lane = lax.broadcasted_iota(jnp.int32, (1, LANES), 1)
    table = jnp.zeros((1, LANES), jnp.float32)
    for step in range(STEPS):
        first, second = (step ^ 2) * tiles, step * tiles
        reduced = jnp.where(c == 0, total[first : first + tiles], total[second : second + tiles])
        adjusted = reduced - carried
        new = (running + adjusted).astype(jnp.bfloat16).astype(jnp.float32)
        carried = (new - running) - adjusted
        running = new
        value = running - carried
        peak = jnp.max(jnp.max(jnp.abs(value), axis=0, keepdims=True), axis=1, keepdims=True)
        table = jnp.where(lane == step * NB + mine, peak, table)
        for t in range(tiles):
            exact[step : step + 1, t * LANES : (t + 1) * LANES] = value[t : t + 1]
    peaks[...] = table


def scale_kernel(place, bucket, exact, tables, units, peaks, compensated):
    mine = bucket[(place[0] * 8 + place[1]) * 2 + place[2]]
    table = jnp.max(tables[...], axis=0, keepdims=True)
    lane = lax.broadcasted_iota(jnp.int32, (STEPS, LANES), 1)
    step = lax.broadcasted_iota(jnp.int32, (STEPS, LANES), 0)
    spot = lane == step * NB + mine
    peak = jnp.max(jnp.where(spot, jnp.broadcast_to(table, spot.shape), 0.0), axis=1, keepdims=True)
    compensated[...] = exact[STEPS - 1 : STEPS, :]
    units[...] = (exact[...] / (peak + EPSILON)).astype(units.dtype)
    for s in range(STEPS):
        peaks[s : s + 1, :] = table[:, s * NB : (s + 1) * NB]


def on_device(grad_codes, exponents, accumulated, arrival, bucket_of_row):
    columns = accumulated.shape[1]
    tiles = columns // LANES
    base, _ = where_rows(tiles)
    place = jnp.stack([lax.axis_index("x"), lax.axis_index("z"), lax.axis_index("c")])
    nz = lax.axis_size("z")
    vmem = pl.BlockSpec(memory_space=pltpu.VMEM)
    smem = pl.BlockSpec(memory_space=pltpu.SMEM)
    codes = grad_codes[:, 0]

    def wide(rows):
        return jnp.pad(rows, ((0, 0), (0, LANES - rows.shape[1])))

    words = jnp.concatenate([wide(exponents[:, 0]), wide(arrival[None]), wide(bucket_of_row[None])])
    picks = pl.pallas_call(
        picks_kernel,
        out_shape=jax.ShapeDtypeStruct((STEPS, ROWS, ROWS), jnp.bfloat16),
        in_specs=[smem, vmem],
        out_specs=vmem,
        compiler_params=room(4),
        cost_estimate=pl.CostEstimate(flops=3 * 10**9, bytes_accessed=10**5, transcendentals=0),
        name="picks",
    )(place, words)

    swap = [(0, 1), (1, 0)]
    mine0, send0 = spread(0, place, picks, codes)
    got0 = lax.ppermute(send0, "c", swap)
    mine1, send1 = spread(1, place, picks, codes)
    got1 = lax.ppermute(send1, "c", swap)
    mine, got = (mine0, mine1), (got0, got1)
    turn = []
    for z in range(nz):
        turn.append((2 * z, 2 * ((z + 1) % nz)))
        turn.append((2 * z + 1, 2 * ((z - 1) % nz) + 1))

    ring = [()] * STEPS
    for hops, rel in PIECES:
        late, first = base[hops, rel]
        ins = (mine[late], got[late]) + ring[rel]
        held = pl.pallas_call(
            functools.partial(add_kernel, first),
            out_shape=jax.ShapeDtypeStruct((8 * tiles, LANES), jnp.float32),
            in_specs=[vmem] * len(ins),
            out_specs=vmem,
            compiler_params=room(4),
            name="add",
        )(*ins)
        ring[rel] = (lax.ppermute(held, ("z", "c"), turn),)
    ring = [arrived for (arrived,) in ring]
    back = [lax.ppermute(arrived, "c", swap) for arrived in ring]
    piece = jax.ShapeDtypeStruct((STEPS * tiles, LANES), jnp.float32)
    own = tuple(base[0, rel][1] for rel in range(STEPS))
    pieces = pl.pallas_call(
        functools.partial(join_kernel, tiles, own),
        out_shape=(piece,) * 4,
        in_specs=[vmem] * 10,
        out_specs=(vmem,) * 4,
        compiler_params=room(4),
        name="join",
    )(mine1, got1, *ring, *back)
    totals = [pieces[0]]
    for k in range(1, 4):
        totals.append(lax.ppermute(pieces[k], "x", [(i, i ^ k) for i in range(4)]))
    exact, table = pl.pallas_call(
        functools.partial(chain_kernel, tiles),
        out_shape=(
            jax.ShapeDtypeStruct((STEPS, columns), jnp.float32),
            jax.ShapeDtypeStruct((1, LANES), jnp.float32),
        ),
        in_specs=[smem, smem] + [vmem] * 5,
        out_specs=(vmem,) * 2,
        compiler_params=room(4),
        name="chain",
    )(place, bucket_of_row, *totals, accumulated.reshape(tiles, LANES))
    table = jnp.maximum(table, lax.ppermute(table, "c", swap))
    count = lax.axis_size(("x", "z", "y"))
    copies = jnp.broadcast_to(table[None], (count, 1, LANES))
    tables = lax.all_to_all(copies, ("x", "z", "y"), 0, 0, tiled=True)
    units, peaks, compensated = pl.pallas_call(
        scale_kernel,
        out_shape=(
            jax.ShapeDtypeStruct((STEPS, columns), jnp.bfloat16),
            jax.ShapeDtypeStruct((STEPS, NB), jnp.float32),
            jax.ShapeDtypeStruct((1, columns), jnp.float32),
        ),
        in_specs=[smem, smem] + [vmem] * 2,
        out_specs=(vmem,) * 3,
        compiler_params=room(4),
        name="scale",
    )(place, bucket_of_row, exact, tables.reshape(count, LANES))
    return units[:, None, :], peaks, compensated


def solution(mesh):
    finer = Mesh(mesh.devices.reshape(4, 8, 2, mesh.shape["tensor"]), ("x", "z", "c", "y"))
    dp = ("x", "z", "c")
    in_specs = (P(None, dp, None, "y"), P(None, dp, None), P(dp, "y"), P(), P())
    out_specs = (P(None, dp, "y"), P(), P(dp, "y"))

    return jax.shard_map(
        on_device, mesh=finer, in_specs=in_specs, out_specs=out_specs, check_vma=False
    )
```

```python
import functools

import jax
import jax.numpy as jnp
from jax import lax
from jax.experimental import pallas as pl
from jax.experimental.pallas import tpu as pltpu
from jax.sharding import Mesh
from jax.sharding import PartitionSpec as P


NB = 16
STEPS = 4
ROWS = 64
LANES = 128
EPSILON = 1e-06

PIECES = tuple(
    (hops - (rel >= 2), rel) for hops in (4, 3, 2, 1) for rel in range(STEPS) if hops - (rel >= 2) > 0
)
FIRST, SECOND = PIECES[:2], PIECES[2:STEPS]


def room(mib):
    return pltpu.CompilerParams(vmem_limit_bytes=mib * 2**20)


def where_rows(tiles):
    base, sizes = {}, [0, 0, 0]
    for piece in PIECES + tuple((0, rel) for rel in range(STEPS)):
        kind = 0 if piece in FIRST else 1 if piece in SECOND else 2
        base[piece] = (kind, sizes[kind])
        sizes[kind] += (8 if piece[0] else 4) * tiles
    return base, sizes


def group_order(rel):
    first = [4, 5] if rel < 2 else [3, 4]
    return first + [k for k in range(8) if k not in first]


def rows_kernel(place, rows):
    x, z, c = place[0], place[1], place[2]
    shape = (ROWS, ROWS)
    group = lax.broadcasted_iota(jnp.int32, shape, 0) // 8
    g = lax.broadcasted_iota(jnp.int32, shape, 0) % 8
    to_x = x ^ (g % 4)
    for rel in range(STEPS):
        k = jnp.zeros(shape, jnp.int32)
        for index, value in enumerate(group_order(rel)):
            k = jnp.where(group == index, value, k)
        to_z = (z + k * (1 - 2 * c)) & 7
        owner = jnp.where(k <= (4 if rel < 2 else 3), c, 1 - c)
        rows[rel] = (to_x * 8 + to_z) * 2 + (owner ^ (g // 4))


def picks_kernel(place, rows, table, picks):
    c = place[2]
    lane = lax.broadcasted_iota(jnp.int32, (ROWS, ROWS), 1)
    arrival, bucket = table[STEPS : STEPS + 1, 0:ROWS], table[STEPS + 1 : STEPS + 2, 0:ROWS]
    for rel in range(STEPS):
        ids = rows[rel]
        row_bucket = jnp.sum(jnp.where(ids == lane, bucket, 0), axis=1, keepdims=True)
        exponents = jnp.where(c == 0, table[rel ^ 2, 0:ROWS][None], table[rel, 0:ROWS][None])
        power = jnp.sum(jnp.where(row_bucket == lane, exponents, 0), axis=1, keepdims=True)
        factor = jnp.ones((ROWS, 1), jnp.float32)
        for bit in range(6):
            factor = factor * jnp.where((power >> bit) & 1 == 1, 2.0 ** -(2**bit), 1.0)
        picks[rel] = jnp.where(ids == arrival, factor, 0.0).astype(jnp.bfloat16)


def spread_kernel(tiles, late, place, picks, codes, *outs):
    base, _ = where_rows(tiles)
    c = place[2]
    width = 2 * LANES
    rows = slice(16, ROWS) if late else slice(0, 16)

    kinds = (2,) if late else (0, 1)
    mine, send = dict(zip(kinds, outs[: len(kinds)])), dict(zip(kinds, outs[len(kinds) :]))

    def put(arrays, piece, at, value):
        kind, first = base[piece]
        arrays[kind][pl.ds(first + at, value.shape[0], tiles), :] = value

    for rel in range(STEPS):
        order = group_order(rel)[2:] if late else group_order(rel)[:2]
        pick = picks[rel, rows, :]
        step = rel ^ (2 * (1 - c))
        for block in range(tiles * LANES // width):
            part = jnp.dot(
                pick,
                codes[step, :, block * width : (block + 1) * width],
                preferred_element_type=jnp.float32,
            )
            for sub in range(2):
                at = 2 * block + sub
                for index, k in enumerate(order):
                    piece = part[index * 8 : index * 8 + 8, sub * LANES : (sub + 1) * LANES]
                    if k == 0:
                        put(mine, (0, rel), at, piece[0:4])
                        put(send, (0, rel ^ 2), at, piece[4:8])
                    elif (k, rel) in base:
                        put(mine, (k, rel), at, piece)
                    else:
                        put(send, (8 - k, rel ^ 2), at, piece)


def spread(late, place, picks, codes):
    tiles = codes.shape[2] // LANES
    sizes = where_rows(tiles)[1]
    shapes = tuple(
        jax.ShapeDtypeStruct((size, LANES), jnp.float32) for size in (sizes[2:] if late else sizes[:2])
    )
    vmem = pl.BlockSpec(memory_space=pltpu.VMEM)
    return pl.pallas_call(
        functools.partial(spread_kernel, tiles, late),
        out_shape=shapes + shapes,
        in_specs=[pl.BlockSpec(memory_space=pltpu.SMEM), vmem, vmem],
        out_specs=(vmem,) * (2 * len(shapes)),
        compiler_params=room(8),
        name="spread",
    )(place, picks, codes)


def add_kernel(first, *refs):
    *ins, out = refs
    rows = slice(first, first + out.shape[0])
    total = ins[0][rows] + ins[1][rows]
    if len(ins) == 3:
        total = total + ins[2][...]
    out[...] = total


def join_kernel(tiles, own, mine, got, r0, r1, r2, r3, b0, b1, b2, b3, *outs):
    ring, back = (r0, r1, r2, r3), (b0, b1, b2, b3)
    for k in range(4):
        rows = slice(k * tiles, (k + 1) * tiles)
        other = slice((k + 4) * tiles, (k + 5) * tiles)
        for rel in range(STEPS):
            at = slice(own[rel] + k * tiles, own[rel] + (k + 1) * tiles)
            outs[k][rel * tiles : (rel + 1) * tiles] = (
                mine[at] + got[at] + ring[rel][rows] + back[rel ^ 2][other]
            )


def chain_kernel(tiles, place, bucket, t0, t1, t2, t3, start, exact, peaks):
    c = place[2]
    mine = bucket[(place[0] * 8 + place[1]) * 2 + c]
    total = t0[...] + t1[...] + t2[...] + t3[...]
    running = start[...].astype(jnp.float32)
    carried = jnp.zeros_like(running)
    lane = lax.broadcasted_iota(jnp.int32, (1, LANES), 1)
    table = jnp.zeros((1, LANES), jnp.float32)
    for step in range(STEPS):
        first, second = (step ^ 2) * tiles, step * tiles
        reduced = jnp.where(c == 0, total[first : first + tiles], total[second : second + tiles])
        adjusted = reduced - carried
        new = (running + adjusted).astype(jnp.bfloat16).astype(jnp.float32)
        carried = (new - running) - adjusted
        running = new
        value = running - carried
        peak = jnp.max(jnp.max(jnp.abs(value), axis=0, keepdims=True), axis=1, keepdims=True)
        table = jnp.where(lane == step * NB + mine, peak, table)
        for t in range(tiles):
            exact[step : step + 1, t * LANES : (t + 1) * LANES] = value[t : t + 1]
    peaks[...] = table


def scale_kernel(place, bucket, exact, tables, units, peaks, compensated):
    mine = bucket[(place[0] * 8 + place[1]) * 2 + place[2]]
    table = jnp.max(tables[...], axis=0, keepdims=True)
    lane = lax.broadcasted_iota(jnp.int32, (STEPS, LANES), 1)
    step = lax.broadcasted_iota(jnp.int32, (STEPS, LANES), 0)
    spot = lane == step * NB + mine
    peak = jnp.max(jnp.where(spot, jnp.broadcast_to(table, spot.shape), 0.0), axis=1, keepdims=True)
    compensated[...] = exact[STEPS - 1 : STEPS, :]
    units[...] = (exact[...] / (peak + EPSILON)).astype(units.dtype)
    for s in range(STEPS):
        peaks[s : s + 1, :] = table[:, s * NB : (s + 1) * NB]


def on_device(grad_codes, exponents, accumulated, arrival, bucket_of_row):
    columns = accumulated.shape[1]
    tiles = columns // LANES
    base, _ = where_rows(tiles)
    place = jnp.stack([lax.axis_index("x"), lax.axis_index("z"), lax.axis_index("c")])
    nz = lax.axis_size("z")
    vmem = pl.BlockSpec(memory_space=pltpu.VMEM)
    smem = pl.BlockSpec(memory_space=pltpu.SMEM)
    codes = grad_codes[:, 0]

    def wide(rows):
        return jnp.pad(rows, ((0, 0), (0, LANES - rows.shape[1])))

    words = jnp.concatenate([wide(exponents[:, 0]), wide(arrival[None]), wide(bucket_of_row[None])])
    rows = pl.pallas_call(
        rows_kernel,
        out_shape=jax.ShapeDtypeStruct((STEPS, ROWS, ROWS), jnp.int32),
        in_specs=[smem],
        out_specs=vmem,
        compiler_params=room(4),
        cost_estimate=pl.CostEstimate(flops=3 * 10**9, bytes_accessed=10**5, transcendentals=0),
        name="rows",
    )(place)
    picks = pl.pallas_call(
        picks_kernel,
        out_shape=jax.ShapeDtypeStruct((STEPS, ROWS, ROWS), jnp.bfloat16),
        in_specs=[smem, vmem, vmem],
        out_specs=vmem,
        compiler_params=room(4),
        name="picks",
    )(place, rows, words)

    swap = [(0, 1), (1, 0)]
    mine0, mine1, send0, send1 = spread(0, place, picks, codes)
    got0 = lax.ppermute(send0, "c", swap)
    got1 = lax.ppermute(send1, "c", swap)
    mine2, send2 = spread(1, place, picks, codes)
    got2 = lax.ppermute(send2, "c", swap)
    mine, got = (mine0, mine1, mine2), (got0, got1, got2)
    turn = []
    for z in range(nz):
        turn.append((2 * z, 2 * ((z + 1) % nz)))
        turn.append((2 * z + 1, 2 * ((z - 1) % nz) + 1))

    ring = [()] * STEPS
    for hops, rel in PIECES:
        late, first = base[hops, rel]
        ins = (mine[late], got[late]) + ring[rel]
        held = pl.pallas_call(
            functools.partial(add_kernel, first),
            out_shape=jax.ShapeDtypeStruct((8 * tiles, LANES), jnp.float32),
            in_specs=[vmem] * len(ins),
            out_specs=vmem,
            compiler_params=room(4),
            name="add",
        )(*ins)
        ring[rel] = (lax.ppermute(held, ("z", "c"), turn),)
    ring = [arrived for (arrived,) in ring]
    back = [lax.ppermute(arrived, "c", swap) for arrived in ring]
    piece = jax.ShapeDtypeStruct((STEPS * tiles, LANES), jnp.float32)
    own = tuple(base[0, rel][1] for rel in range(STEPS))
    pieces = pl.pallas_call(
        functools.partial(join_kernel, tiles, own),
        out_shape=(piece,) * 4,
        in_specs=[vmem] * 10,
        out_specs=(vmem,) * 4,
        compiler_params=room(4),
        name="join",
    )(mine2, got2, *ring, *back)
    totals = [pieces[0]]
    for k in range(1, 4):
        totals.append(lax.ppermute(pieces[k], "x", [(i, i ^ k) for i in range(4)]))
    exact, table = pl.pallas_call(
        functools.partial(chain_kernel, tiles),
        out_shape=(
            jax.ShapeDtypeStruct((STEPS, columns), jnp.float32),
            jax.ShapeDtypeStruct((1, LANES), jnp.float32),
        ),
        in_specs=[smem, smem] + [vmem] * 5,
        out_specs=(vmem,) * 2,
        compiler_params=room(4),
        name="chain",
    )(place, bucket_of_row, *totals, accumulated.reshape(tiles, LANES))
    table = jnp.maximum(table, lax.ppermute(table, "c", swap))
    count = lax.axis_size(("x", "z", "y"))
    copies = jnp.broadcast_to(table[None], (count, 1, LANES))
    tables = lax.all_to_all(copies, ("x", "z", "y"), 0, 0, tiled=True)
    units, peaks, compensated = pl.pallas_call(
        scale_kernel,
        out_shape=(
            jax.ShapeDtypeStruct((STEPS, columns), jnp.bfloat16),
            jax.ShapeDtypeStruct((STEPS, NB), jnp.float32),
            jax.ShapeDtypeStruct((1, columns), jnp.float32),
        ),
        in_specs=[smem, smem] + [vmem] * 2,
        out_specs=(vmem,) * 3,
        compiler_params=room(4),
        name="scale",
    )(place, bucket_of_row, exact, tables.reshape(count, LANES))
    return units[:, None, :], peaks, compensated


def solution(mesh):
    finer = Mesh(mesh.devices.reshape(4, 8, 2, mesh.shape["tensor"]), ("x", "z", "c", "y"))
    dp = ("x", "z", "c")
    in_specs = (P(None, dp, None, "y"), P(None, dp, None), P(dp, "y"), P(), P())
    out_specs = (P(None, dp, "y"), P(), P(dp, "y"))

    return jax.shard_map(on_device, mesh=finer, in_specs=in_specs, out_specs=out_specs, check_vma=False)
```
